32 devices in a mesh: slides: 2 (over y), row: 16 (over z, x, core).
Axes of the slice: x: 2, y: 2, z: 4, core: 2. Of those that a mesh axis runs over, the one named last changes fastest.
Arguments:
- slide_pixels: bfloat16 [2048, 16384], P(('slides', 'row')), parts along dimension 0, may hold values from -6 to 6
- tissue_mask: int32 [64, 8], P(('slides', 'row')), parts along dimension 0, may hold values from 0 to 1, as said below
- conv_weight: bfloat16 [3, 3, 64, 64], replicated, may hold values from -0.25 to 0.25
- conv_bias: bfloat16 [64], replicated, may hold values from -3 to 3
Outputs:
- packed_tiles: bfloat16 [256, 32, 2048], P(('slides', 'row')), parts along dimension 0
The draws below stay inside these ranges and needn't reach their ends.
There are 2 independent parts, one for each index of `slides`. The reference program is written for one: setup_inputs(seed, part) draws one part's arguments, and reference() takes and returns one part's arrays. A program takes and returns all parts, laid end to end along the dimension named above; an argument that names none is the same for every part. Nothing has to cross between parts.
Inputs may be any that keep to these rules, and one draw needn't show every extreme that they name: `tissue_mask`: exactly 128 tiles hold tissue. For every s from 1 to 15, the first s * 2 tile rows hold s * 8 + e tissue tiles with e between 0 and 2; e = 2 occurs in every draw. For every such s, some column holds tissue in both tile row s * 2 - 1 and tile row s * 2.
All inputs are finite; a program needn't handle non-finite values.
Results may differ from the reference program's by a relative error of at most 0.001.
Values may be sent and summed in bfloat16 or wider, within the bound.
A program may use at most 64 MiB of HBM per device.

```python
import jax
import jax.numpy as jnp
from jax import lax

CH = 64
SIDE = 32
SLOTS = 8
ROWS_DEV = 2
COLS = 8
SHIFT_MOST = 2
GRID_ROWS = 32
N_ROW = 16


def draw_tissue_mask(key, part):
    walk_key, first_key, order_key, column_key = jax.random.split(jax.random.fold_in(key, 7), 4)
    device_total = N_ROW
    reach_most = SHIFT_MOST
    drift_walk = jax.random.randint(walk_key, (device_total + 1,), 0, reach_most + 1)
    first_step = jax.random.randint(first_key, (), 1, device_total)
    step_index = jnp.arange(device_total + 1)
    drift_walk = jnp.where(step_index == first_step, reach_most, drift_walk)
    middle = device_total // 2
    in_window = (step_index >= middle - 2) & (step_index <= middle + 3)
    alternating = step_index % 2 * reach_most
    drift_walk = jnp.where(in_window, alternating, drift_walk)
    drift_walk = jnp.where((step_index == 0) | (step_index == device_total), 0, drift_walk)
    counts = SLOTS + drift_walk[1:] - drift_walk[:-1]
    tiles_band = ROWS_DEV * COLS
    boundary_cols = jax.random.randint(column_key, (device_total + 1,), 0, COLS)
    tile_index = jnp.arange(tiles_band)
    top_forced = tile_index[None, :] == boundary_cols[:-1, None]
    bottom_forced = tile_index[None, :] == (ROWS_DEV - 1) * COLS + boundary_cols[1:, None]
    band_index = jnp.arange(device_total)[:, None]
    forced = top_forced & (band_index > 0) | bottom_forced & (band_index < device_total - 1)
    scores = jax.random.randint(order_key, (device_total, tiles_band), 0, 1 << 20) * tiles_band
    scores = scores + tile_index[None, :]
    scores = jnp.where(forced, -1 - tile_index[None, :], scores)
    ranking = jnp.argsort(jnp.argsort(scores, axis=1), axis=1)
    tissue = (ranking < counts[:, None]).astype(jnp.int32)
    return tissue.reshape(device_total * ROWS_DEV, COLS)


def steps_of(key, dims, cuts, smallest, largest):
    loudness, own = 1.0, jax.random.fold_in(key, 6)
    for dim, parts in cuts:
        steps = jnp.exp(jax.random.uniform(jax.random.fold_in(own, dim), (parts,), jnp.float32, smallest / len(cuts), largest / len(cuts)))
        loudness = loudness * jnp.repeat(steps, dims[dim] // parts).reshape([-1 if axis == dim else 1 for axis in range(len(dims))])
    return loudness


def noise(stream_key, extent, width, bound, cuts=(), held_as=jnp.bfloat16):
    loudness = steps_of(stream_key, extent, cuts, -0.22, 0.18) if cuts else 1.0
    array = jax.random.normal(stream_key, extent, jnp.float32) * width * loudness
    return jnp.minimum(jnp.maximum(array, -bound), bound).astype(held_as)


def setup_inputs(seed: int = 0, part: int = 0) -> dict:
    key_of = jax.random.split(jax.random.key(seed), 5)
    own_keys = jax.random.split(jax.random.fold_in(key_of[4], part), 5)
    slide_pixels = noise(own_keys[0], (GRID_ROWS * SIDE, COLS * SIDE * CH), 1.0, 6.0, ((0, 16),))
    tissue_mask = draw_tissue_mask(jax.random.fold_in(jax.random.fold_in(key_of[4], part), 71), part)
    conv_weight = noise(key_of[2], (3, 3, CH, CH), (9 * CH) ** -0.5, 0.25)
    conv_bias = noise(key_of[3], (CH,), 0.5, 3.0)
    return dict(slide_pixels=slide_pixels, tissue_mask=tissue_mask, conv_weight=conv_weight, conv_bias=conv_bias)


def reference(slide_pixels, tissue_mask, conv_weight, conv_bias):
    grid_rows, grid_cols = tissue_mask.shape
    channels = conv_weight.shape[2]
    side = slide_pixels.shape[0] // grid_rows
    image = slide_pixels.reshape(grid_rows * side, grid_cols * side, channels)
    flat_mask = tissue_mask.reshape(grid_rows * grid_cols)
    order = jnp.argsort(1 - flat_mask, stable=True)[: N_ROW * SLOTS].astype(jnp.int32)
    weight_full = conv_weight.astype(jnp.float32)
    bias_full = conv_bias.astype(jnp.float32)

    def one_tile(position):
        tile_row = position // grid_cols
        tile_col = position % grid_cols
        offsets = jnp.arange(side + 2, dtype=jnp.int32) - 1
        pixel_rows = tile_row * side + offsets
        pixel_cols = tile_col * side + offsets
        row_inside = (pixel_rows >= 0) & (pixel_rows < grid_rows * side)
        col_inside = (pixel_cols >= 0) & (pixel_cols < grid_cols * side)
        rows_safe = jnp.clip(pixel_rows, 0, grid_rows * side - 1).astype(jnp.int32)
        cols_safe = jnp.clip(pixel_cols, 0, grid_cols * side - 1).astype(jnp.int32)
        window = jnp.take(jnp.take(image, rows_safe, axis=0), cols_safe, axis=1).astype(jnp.float32)
        tissue = jnp.take(jnp.take(tissue_mask, rows_safe // side, axis=0), cols_safe // side, axis=1)
        living = row_inside[:, None] & col_inside[None, :] & (tissue == 1)
        window = jnp.where(living[:, :, None], window, jnp.zeros_like(window))
        result = jnp.zeros((side, side, channels), jnp.float32)
        for vertical in range(3):
            for horizontal in range(3):
                result = result + jnp.einsum(
                    "hwc,co->hwo",
                    window[vertical:vertical + side, horizontal:horizontal + side],
                    weight_full[vertical, horizontal],
                    precision=lax.Precision.HIGHEST)
        result = result + bias_full
        return result.astype(jnp.bfloat16).reshape(side, side * channels)

    return lax.map(one_tile, order)
```

```python
import functools

import jax
import jax.numpy as jnp
from jax import lax
from jax.experimental import pallas as pl
from jax.experimental.pallas import tpu as pltpu
from jax.sharding import PartitionSpec as P

SLOTS = 8
SHIFT_MOST = 2
LANES = 128
PACK = 16
MESH = pl.DeviceIdType.MESH


def kernel(
    n, side, channels,
    x_ref, mask_s, mask_v, w_ref, b_ref, out_ref,
    image, conv, low, rows3, wide, masks, stage_up, stage_dn, halo_top, halo_bot, onward, arrived,
    x_sem, mask_send, mask_recv, halo_send, halo_recv, tile_send, tile_recv,
):
    band_rows, cols = mask_s.shape
    height = band_rows * side
    width = side * channels
    tiles = band_rows * cols
    quad = 2 * LANES
    groups = width // quad
    per = quad // channels
    half = LANES // channels
    me = lax.axis_index("row")

    def fetch(c):
        return pltpu.make_async_copy(
            x_ref.at[:, pl.ds(c * width, width)],
            image.at[pl.ds(PACK, height), pl.ds(LANES + c * width, width)],
            x_sem.at[c],
        )

    for c in range(cols):
        fetch(c).start()

    barrier = pltpu.get_barrier_semaphore()

    def greet(j, carry):
        pl.semaphore_signal(
            barrier, inc=1, device_id={"row": lax.rem(me + j, n)}, device_id_type=MESH
        )
        return carry

    lax.fori_loop(1, n, greet, 0)

    none = jnp.zeros((channels, channels), jnp.bfloat16)
    for dy in range(3):
        taps = [w_ref[dy, 0], w_ref[dy, 1], w_ref[dy, 2]]
        for p in range(2 * per):
            for q in range(per // half):
                u = p - half - half * q
                parts = [taps[u + 1 - o] if 0 <= u + 1 - o <= 2 else none for o in range(half)]
                wide[dy, p * channels:(p + 1) * channels, q * LANES:(q + 1) * LANES] = (
                    jnp.concatenate(parts, axis=1)
                )
    edge = jnp.zeros((height + 2 * PACK, LANES), jnp.bfloat16)
    image[:, 0:LANES] = edge
    image[:, LANES + cols * width:2 * LANES + cols * width] = edge
    masks[me] = mask_v[...]
    blank_rows = jnp.zeros((PACK, cols * width), jnp.bfloat16)
    image[0:PACK, LANES:LANES + cols * width] = blank_rows
    image[PACK + height:2 * PACK + height, LANES:LANES + cols * width] = blank_rows

    firsts, lasts = [], []
    for c in range(cols):
        fetch(c).wait()
        for r in range(band_rows):
            keep = jnp.full((side, LANES), mask_s[r, c], jnp.int32).astype(jnp.float32)
            keep = keep.astype(jnp.bfloat16)
            for k in range(width // LANES):
                at = (pl.ds(PACK + r * side, side), pl.ds(LANES + c * width + k * LANES, LANES))
                image[at] = image[at] * keep
        span = pl.ds(LANES + c * width, width)
        first = image[PACK:2 * PACK, span].astype(jnp.float32)
        last = image[height:height + PACK, span].astype(jnp.float32)
        firsts.append(first[0:1])
        lasts.append(last[PACK - 1:PACK])
    stage_up[...] = jnp.concatenate(firsts, axis=0).astype(jnp.bfloat16)
    stage_dn[...] = jnp.concatenate(lasts, axis=0).astype(jnp.bfloat16)

    pl.semaphore_wait(barrier, n - 1)

    down = pltpu.make_async_remote_copy(
        stage_dn, halo_top, halo_send.at[0], halo_recv.at[0],
        device_id={"row": lax.rem(me + 1, n)}, device_id_type=MESH)
    up = pltpu.make_async_remote_copy(
        stage_up, halo_bot, halo_send.at[1], halo_recv.at[1],
        device_id={"row": lax.rem(me + n - 1, n)}, device_id_type=MESH)
    is_first = me == 0
    is_last = me == n - 1

    @pl.when(jnp.logical_not(is_last))
    def _():
        down.start()

    @pl.when(jnp.logical_not(is_first))
    def _():
        up.start()

    def mask_copy(target, slot):
        return pltpu.make_async_remote_copy(
            mask_v, masks.at[slot], mask_send.at[target], mask_recv.at[slot],
            device_id={"row": target}, device_id_type=MESH)

    def tell(j, carry):
        mask_copy(lax.rem(me + j, n), me).start()
        return carry

    lax.fori_loop(1, n, tell, 0)

    bias = b_ref[...].astype(jnp.float32)
    bias = jnp.concatenate([bias] * per, axis=1)
    duo = 2
    duos = cols // duo
    bands = duo * groups

    def convolve(r, pair, carry):
        left = pl.multiple_of(pair * (duo * width), duo * width)
        for k in range(bands + 1):
            block = image[r * side:(r + 1) * side + 2 * PACK, pl.ds(left + k * quad, quad)]
            span = pl.ds(k * quad, quad)
            block32 = block.astype(jnp.float32)
            rows3[0, :, span] = block32[PACK - 1:PACK - 1 + side].astype(jnp.bfloat16)
            rows3[1, :, span] = block[PACK:PACK + side]
            rows3[2, :, span] = block32[PACK + 1:PACK + 1 + side].astype(jnp.bfloat16)
        total = jnp.broadcast_to(bias, (bands * side, quad))
        for dy in range(3):
            left_side = jnp.concatenate(
                [rows3[dy, :, g * quad:(g + 2) * quad] for g in range(bands)], axis=0)
            total = total + jnp.dot(
                left_side, wide[dy], preferred_element_type=jnp.float32)
        done = total.astype(jnp.bfloat16)
        for g in range(bands):
            at = g % groups * quad
            tile_at = r * cols + pair * duo + g // groups
            conv[tile_at, :, at:at + quad] = done[g * side:(g + 1) * side]
            if r == band_rows - 1:
                low[pair * duo + g // groups, :, at:at + quad] = (
                    total[(g + 1) * side - 8:(g + 1) * side])
        return carry

    lax.fori_loop(0, duos, functools.partial(convolve, band_rows - 1), 0)

    @pl.when(jnp.logical_not(is_first))
    def _():
        down.wait_recv()
        lines = halo_top[...].astype(jnp.float32)
        for c in range(cols):
            image[0:PACK, LANES + c * width:LANES + (c + 1) * width] = (
                jnp.broadcast_to(lines[c:c + 1], (PACK, width)).astype(jnp.bfloat16))

    for r in range(band_rows - 2, 0, -1):
        lax.fori_loop(0, duos, functools.partial(convolve, r), 0)
    lax.fori_loop(duos - 1, duos, functools.partial(convolve, 0), 0)

    @pl.when(jnp.logical_not(is_last))
    def _():
        up.wait_recv()
        lines = halo_bot[...].astype(jnp.float32)
        blank = jnp.zeros((1, LANES), jnp.float32)
        before = jnp.concatenate([blank, lines[0:cols - 1, width - LANES:width]], axis=0)
        after = jnp.concatenate([lines[1:cols, 0:LANES], blank], axis=0)
        lines = jnp.concatenate([before, lines, after], axis=1)
        stack = jnp.concatenate(
            [lines[:, g * quad:(g + 2) * quad] for g in range(groups)], axis=0)
        more = jnp.dot(
            stack.astype(jnp.bfloat16), wide[2], preferred_element_type=jnp.float32)
        lowest = lax.broadcasted_iota(jnp.int32, (PACK, quad), 0) == PACK - 1
        for c in range(cols):
            for g in range(groups):
                at = g * quad
                row = low[c, 7:8, at:at + quad] + more[g * cols + c:g * cols + c + 1]
                where = ((band_rows - 1) * cols + c, pl.ds(side - PACK, PACK), pl.ds(at, quad))
                old = conv[where].astype(jnp.float32)
                new = jnp.where(lowest, jnp.broadcast_to(row, (PACK, quad)), old)
                conv[where] = new.astype(jnp.bfloat16)

    def told(j, carry):
        mask_copy(lax.rem(me + j, n), lax.rem(me + j, n)).wait_recv()
        return carry

    lax.fori_loop(1, n, told, 0)
    device = lax.broadcasted_iota(jnp.int32, masks.shape, 0)
    excess = jnp.sum(jnp.where(device < me, masks[...], 0)) - SLOTS * me
    seen = []
    for r in range(band_rows):
        for c in range(cols):
            seen.append(mask_s[r, c] + (seen[-1] if seen else 0))

    def place(rank):
        total = jnp.int32(0)
        for count in seen:
            total = total + jnp.where(count <= rank, 1, 0)
        return jnp.minimum(total, tiles - 1)

    for k in range(SHIFT_MOST):
        onward[k] = conv[place(SLOTS + k - excess)]
    tile = pltpu.make_async_remote_copy(
        onward, arrived, tile_send, tile_recv,
        device_id={"row": lax.rem(me + 1, n)}, device_id_type=MESH)

    @pl.when(jnp.logical_not(is_last))
    def _():
        tile.start()

    lax.fori_loop(0, duos - 1, functools.partial(convolve, 0), 0)

    for k in range(SLOTS):
        out_ref[k] = conv[place(k - excess)]

    @pl.when(jnp.logical_not(is_first))
    def _():
        tile.wait_recv()
        for k in range(SHIFT_MOST):
            own = out_ref[k].astype(jnp.float32)
            theirs = arrived[k].astype(jnp.float32)
            late = jnp.full(own.shape, excess, jnp.int32) > k
            out_ref[k] = jnp.where(late, theirs, own).astype(jnp.bfloat16)
        up.wait_send()

    @pl.when(jnp.logical_not(is_last))
    def _():
        down.wait_send()
        tile.wait_send()

    def sent(j, carry):
        mask_copy(lax.rem(me + j, n), me).wait_send()
        return carry

    lax.fori_loop(1, n, sent, 0)


def on_device(slide_pixels, tissue_mask, conv_weight, conv_bias):
    n = lax.axis_size("row")
    band_rows, cols = tissue_mask.shape
    channels = conv_weight.shape[2]
    height = slide_pixels.shape[0]
    side = height // band_rows
    width = side * channels
    quad = 2 * LANES
    vmem = pl.BlockSpec(memory_space=pltpu.VMEM)
    bf16 = jnp.bfloat16
    return pl.pallas_call(
        functools.partial(kernel, n, side, channels),
        out_shape=jax.ShapeDtypeStruct((SLOTS, side, width), bf16),
        in_specs=[
            pl.BlockSpec(memory_space=pl.ANY),
            pl.BlockSpec(memory_space=pltpu.SMEM),
            vmem, vmem, vmem,
        ],
        out_specs=vmem,
        scratch_shapes=[
            pltpu.VMEM((height + 2 * PACK, cols * width + 2 * LANES), bf16),
            pltpu.VMEM((band_rows * cols, side, width), bf16),
            pltpu.VMEM((cols, 8, width), jnp.float32),
            pltpu.VMEM((3, side, 2 * width + quad), bf16),
            pltpu.VMEM((3, 2 * quad, quad), bf16),
            pltpu.VMEM((n, band_rows, cols), jnp.int32),
            pltpu.VMEM((cols, width), bf16),
            pltpu.VMEM((cols, width), bf16),
            pltpu.VMEM((cols, width), bf16),
            pltpu.VMEM((cols, width), bf16),
            pltpu.VMEM((SHIFT_MOST, side, width), bf16),
            pltpu.VMEM((SHIFT_MOST, side, width), bf16),
            pltpu.SemaphoreType.DMA((cols,)),
            pltpu.SemaphoreType.DMA((n,)),
            pltpu.SemaphoreType.DMA((n,)),
            pltpu.SemaphoreType.DMA((2,)),
            pltpu.SemaphoreType.DMA((2,)),
            pltpu.SemaphoreType.DMA,
            pltpu.SemaphoreType.DMA,
        ],
        compiler_params=pltpu.CompilerParams(collective_id=0, has_side_effects=True),
    )(slide_pixels, tissue_mask, tissue_mask, conv_weight, conv_bias.reshape(1, channels))


def solution(mesh):
    return jax.shard_map(
        on_device,
        mesh=mesh,
        in_specs=(P(("slides", "row"), None), P(("slides", "row"), None), P(), P()),
        out_specs=P(("slides", "row"), None, None),
        check_vma=False,
    )
```

```python
import functools

import jax
import jax.numpy as jnp
from jax import lax
from jax.experimental import pallas as pl
from jax.experimental.pallas import tpu as pltpu
from jax.sharding import PartitionSpec as P

SLOTS = 8
SHIFT_MOST = 2
LANES = 128
PACK = 16
MESH = pl.DeviceIdType.MESH


def kernel(
    n, side, channels,
    x_ref, mask_s, mask_v, w_ref, b_ref, out_any,
    image, conv, low, rows3, wide, masks, stage_up, stage_dn, halo_top, halo_bot, onward, arrived,
    x_sem, mask_send, mask_recv, halo_send, halo_recv, tile_send, tile_recv,
    out_ref, out_sem,
):
    band_rows, cols = mask_s.shape
    height = band_rows * side
    width = side * channels
    tiles = band_rows * cols
    quad = 2 * LANES
    groups = width // quad
    per = quad // channels
    half = LANES // channels
    me = lax.axis_index("row")

    barrier = pltpu.get_barrier_semaphore()

    def greet(j, carry):
        pl.semaphore_signal(
            barrier, inc=1, device_id={"row": lax.rem(me + j, n)}, device_id_type=MESH
        )
        return carry

    lax.fori_loop(1, n, greet, 0)

    def fetch(c):
        return pltpu.make_async_copy(
            x_ref.at[:, pl.ds(c * width, width)],
            image.at[pl.ds(PACK, height), pl.ds(LANES + c * width, width)],
            x_sem.at[c],
        )

    for c in range(cols):
        fetch(c).start()

    none = jnp.zeros((channels, channels), jnp.bfloat16)
    for dy in range(3):
        taps = [w_ref[dy, 0], w_ref[dy, 1], w_ref[dy, 2]]
        for p in range(2 * per):
            for q in range(per // half):
                u = p - half - half * q
                parts = [taps[u + 1 - o] if 0 <= u + 1 - o <= 2 else none for o in range(half)]
                wide[dy, p * channels:(p + 1) * channels, q * LANES:(q + 1) * LANES] = (
                    jnp.concatenate(parts, axis=1)
                )
    edge = jnp.zeros((height + 2 * PACK, LANES), jnp.bfloat16)
    image[:, 0:LANES] = edge
    image[:, LANES + cols * width:2 * LANES + cols * width] = edge
    masks[me] = mask_v[...]
    blank_rows = jnp.zeros((PACK, cols * width), jnp.bfloat16)
    image[0:PACK, LANES:LANES + cols * width] = blank_rows
    image[PACK + height:2 * PACK + height, LANES:LANES + cols * width] = blank_rows

    firsts, lasts = [], []
    for c in range(cols):
        fetch(c).wait()
        for r in range(band_rows):
            keep = jnp.full((side, LANES), mask_s[r, c], jnp.int32).astype(jnp.float32)
            keep = keep.astype(jnp.bfloat16)
            for k in range(width // LANES):
                at = (pl.ds(PACK + r * side, side), pl.ds(LANES + c * width + k * LANES, LANES))
                image[at] = image[at] * keep
        span = pl.ds(LANES + c * width, width)
        first = image[PACK:2 * PACK, span].astype(jnp.float32)
        last = image[height:height + PACK, span].astype(jnp.float32)
        firsts.append(first[0:1])
        lasts.append(last[PACK - 1:PACK])
    stage_up[...] = jnp.concatenate(firsts, axis=0).astype(jnp.bfloat16)
    stage_dn[...] = jnp.concatenate(lasts, axis=0).astype(jnp.bfloat16)

    pl.semaphore_wait(barrier, n - 1)

    down = pltpu.make_async_remote_copy(
        stage_dn, halo_top, halo_send.at[0], halo_recv.at[0],
        device_id={"row": lax.rem(me + 1, n)}, device_id_type=MESH)
    up = pltpu.make_async_remote_copy(
        stage_up, halo_bot, halo_send.at[1], halo_recv.at[1],
        device_id={"row": lax.rem(me + n - 1, n)}, device_id_type=MESH)
    is_first = me == 0
    is_last = me == n - 1

    @pl.when(jnp.logical_not(is_last))
    def _():
        down.start()

    @pl.when(jnp.logical_not(is_first))
    def _():
        up.start()

    def mask_copy(target, slot):
        return pltpu.make_async_remote_copy(
            mask_v, masks.at[slot], mask_send.at[target], mask_recv.at[slot],
            device_id={"row": target}, device_id_type=MESH)

    def tell(j, carry):
        mask_copy(lax.rem(me + j, n), me).start()
        return carry

    lax.fori_loop(1, n, tell, 0)

    bias = b_ref[...].astype(jnp.float32)
    bias = jnp.concatenate([bias] * per, axis=1)
    duo = 2
    duos = cols // duo
    bands = duo * groups

    def convolve(r, pair, carry):
        left = pl.multiple_of(pair * (duo * width), duo * width)
        for k in range(bands + 1):
            block = image[r * side:(r + 1) * side + 2 * PACK, pl.ds(left + k * quad, quad)]
            span = pl.ds(k * quad, quad)
            block32 = block.astype(jnp.float32)
            rows3[0, :, span] = block32[PACK - 1:PACK - 1 + side].astype(jnp.bfloat16)
            rows3[1, :, span] = block[PACK:PACK + side]
            rows3[2, :, span] = block32[PACK + 1:PACK + 1 + side].astype(jnp.bfloat16)
        left_side = jnp.concatenate([jnp.concatenate(
            [rows3[dy, :, g * quad:(g + 2) * quad] for g in range(bands)], axis=0)
            for dy in range(3)], axis=1)
        total = jnp.dot(left_side, wide[...].reshape(6 * quad, quad),
            preferred_element_type=jnp.float32) + bias
        done = total.astype(jnp.bfloat16)
        for g in range(bands):
            at = g % groups * quad
            tile_at = r * cols + pair * duo + g // groups
            conv[tile_at, :, at:at + quad] = done[g * side:(g + 1) * side]
            if r == band_rows - 1:
                low[pair * duo + g // groups, :, at:at + quad] = (
                    total[(g + 1) * side - 8:(g + 1) * side])
        return carry

    lax.fori_loop(0, duos, functools.partial(convolve, band_rows - 1), 0)

    @pl.when(jnp.logical_not(is_first))
    def _():
        down.wait_recv()
        lines = halo_top[...].astype(jnp.float32)
        for c in range(cols):
            image[0:PACK, LANES + c * width:LANES + (c + 1) * width] = (
                jnp.broadcast_to(lines[c:c + 1], (PACK, width)).astype(jnp.bfloat16))

    for r in range(band_rows - 2, 0, -1):
        lax.fori_loop(0, duos, functools.partial(convolve, r), 0)
    lax.fori_loop(duos - 1, duos, functools.partial(convolve, 0), 0)

    @pl.when(jnp.logical_not(is_last))
    def _():
        up.wait_recv()
        lines = halo_bot[...].astype(jnp.float32)
        blank = jnp.zeros((1, LANES), jnp.float32)
        before = jnp.concatenate([blank, lines[0:cols - 1, width - LANES:width]], axis=0)
        after = jnp.concatenate([lines[1:cols, 0:LANES], blank], axis=0)
        lines = jnp.concatenate([before, lines, after], axis=1)
        stack = jnp.concatenate(
            [lines[:, g * quad:(g + 2) * quad] for g in range(groups)], axis=0)
        more = jnp.dot(
            stack.astype(jnp.bfloat16), wide[2], preferred_element_type=jnp.float32)
        lowest = lax.broadcasted_iota(jnp.int32, (PACK, quad), 0) == PACK - 1
        for c in range(cols):
            for g in range(groups):
                at = g * quad
                row = low[c, 7:8, at:at + quad] + more[g * cols + c:g * cols + c + 1]
                where = ((band_rows - 1) * cols + c, pl.ds(side - PACK, PACK), pl.ds(at, quad))
                old = conv[where].astype(jnp.float32)
                new = jnp.where(lowest, jnp.broadcast_to(row, (PACK, quad)), old)
                conv[where] = new.astype(jnp.bfloat16)

    seen = []
    for r in range(band_rows):
        for c in range(cols):
            seen.append(mask_s[r, c] + (seen[-1] if seen else 0))

    def place(rank):
        total = jnp.int32(0)
        for count in seen:
            total = total + jnp.where(count <= rank, 1, 0)
        return jnp.minimum(total, tiles - 1)

    for k in range(SHIFT_MOST):
        onward[k] = conv[place(seen[-1] - SHIFT_MOST + k)]
    tile = pltpu.make_async_remote_copy(
        onward, arrived, tile_send, tile_recv,
        device_id={"row": lax.rem(me + 1, n)}, device_id_type=MESH)

    @pl.when(jnp.logical_not(is_last))
    def _():
        tile.start()

    lax.fori_loop(0, duos - 1, functools.partial(convolve, 0), 0)

    def told(j, carry):
        mask_copy(lax.rem(me + j, n), lax.rem(me + j, n)).wait_recv()
        return carry

    lax.fori_loop(1, n, told, 0)
    device = lax.broadcasted_iota(jnp.int32, masks.shape, 0)
    excess = jnp.sum(jnp.where(device < me, masks[...], 0)) - SLOTS * me

    def give(k):
        return pltpu.make_async_copy(out_ref.at[k], out_any.at[k], out_sem.at[k])

    for k in range(SHIFT_MOST, SLOTS):
        out_ref[k] = conv[place(k - excess)]
        give(k).start()
    for k in range(SHIFT_MOST):
        out_ref[k] = conv[place(k - excess)]

    @pl.when(jnp.logical_not(is_first))
    def _():
        tile.wait_recv()
        late_at = [
            jnp.minimum(k + SHIFT_MOST - jnp.clip(excess, 0, SHIFT_MOST), SHIFT_MOST - 1)
            for k in range(SHIFT_MOST)
        ]
        for k in range(SHIFT_MOST):
            own = out_ref[k].astype(jnp.float32)
            theirs = arrived[late_at[k]].astype(jnp.float32)
            late = jnp.full(own.shape, excess, jnp.int32) > k
            out_ref[k] = jnp.where(late, theirs, own).astype(jnp.bfloat16)
        up.wait_send()

    for k in range(SHIFT_MOST):
        give(k).start()

    @pl.when(jnp.logical_not(is_last))
    def _():
        down.wait_send()
        tile.wait_send()

    def sent(j, carry):
        mask_copy(lax.rem(me + j, n), me).wait_send()
        return carry

    lax.fori_loop(1, n, sent, 0)
    for k in range(SLOTS):
        give(k).wait()


def hand_on(in_ref, out_ref, held, in_sem, out_sem):
    def take(k):
        return pltpu.make_async_copy(in_ref.at[k], held.at[k], in_sem.at[k])

    def give(k):
        return pltpu.make_async_copy(held.at[k], out_ref.at[k], out_sem.at[k])

    for k in range(SLOTS):
        take(k).start()
    for k in range(SLOTS):
        take(k).wait()
        give(k).start()
    for k in range(SLOTS):
        give(k).wait()


def on_device(slide_pixels, tissue_mask, conv_weight, conv_bias):
    n = lax.axis_size("row")
    band_rows, cols = tissue_mask.shape
    channels = conv_weight.shape[2]
    height = slide_pixels.shape[0]
    side = height // band_rows
    width = side * channels
    quad = 2 * LANES
    vmem = pl.BlockSpec(memory_space=pltpu.VMEM)
    bf16 = jnp.bfloat16
    tiles = pl.pallas_call(
        functools.partial(kernel, n, side, channels),
        out_shape=jax.ShapeDtypeStruct((SLOTS, side, width), bf16),
        in_specs=[
            pl.BlockSpec(memory_space=pl.ANY),
            pl.BlockSpec(memory_space=pltpu.SMEM),
            vmem, vmem, vmem,
        ],
        out_specs=pl.BlockSpec(memory_space=pl.ANY),
        scratch_shapes=[
            pltpu.VMEM((height + 2 * PACK, cols * width + 2 * LANES), bf16),
            pltpu.VMEM((band_rows * cols, side, width), bf16),
            pltpu.VMEM((cols, 8, width), jnp.float32),
            pltpu.VMEM((3, side, 2 * width + quad), bf16),
            pltpu.VMEM((3, 2 * quad, quad), bf16),
            pltpu.VMEM((n, band_rows, cols), jnp.int32),
            pltpu.VMEM((cols, width), bf16),
            pltpu.VMEM((cols, width), bf16),
            pltpu.VMEM((cols, width), bf16),
            pltpu.VMEM((cols, width), bf16),
            pltpu.VMEM((SHIFT_MOST, side, width), bf16),
            pltpu.VMEM((SHIFT_MOST, side, width), bf16),
            pltpu.SemaphoreType.DMA((cols,)),
            pltpu.SemaphoreType.DMA((n,)),
            pltpu.SemaphoreType.DMA((n,)),
            pltpu.SemaphoreType.DMA((2,)),
            pltpu.SemaphoreType.DMA((2,)),
            pltpu.SemaphoreType.DMA,
            pltpu.SemaphoreType.DMA,
            pltpu.VMEM((SLOTS, side, width), bf16),
            pltpu.SemaphoreType.DMA((SLOTS,)),
        ],
        compiler_params=pltpu.CompilerParams(collective_id=0, has_side_effects=True),
    )(slide_pixels, tissue_mask, tissue_mask, conv_weight, conv_bias.reshape(1, channels))
    return pl.pallas_call(
        hand_on,
        out_shape=jax.ShapeDtypeStruct(tiles.shape, bf16),
        in_specs=[pl.BlockSpec(memory_space=pl.ANY)],
        out_specs=pl.BlockSpec(memory_space=pl.ANY),
        scratch_shapes=[
            pltpu.VMEM(tiles.shape, bf16),
            pltpu.SemaphoreType.DMA((SLOTS,)),
            pltpu.SemaphoreType.DMA((SLOTS,)),
        ],
    )(tiles)


def solution(mesh):
    return jax.shard_map(
        on_device,
        mesh=mesh,
        in_specs=(P(("slides", "row"), None), P(("slides", "row"), None), P(), P()),
        out_specs=P(("slides", "row"), None, None),
        check_vma=False,
    )
```

```python
import functools

import jax
import jax.numpy as jnp
from jax import lax
from jax.experimental import pallas as pl
from jax.experimental.pallas import tpu as pltpu
from jax.sharding import PartitionSpec as P

SLOTS = 8
SHIFT_MOST = 2
LANES = 128
PACK = 16
MESH = pl.DeviceIdType.MESH


def kernel(
    n, side, channels,
    x_ref, mask_s, mask_v, w_ref, b_ref, out_any,
    image, conv, low, rows3, wide, masks, stage_up, stage_dn, halo_top, halo_bot, onward, arrived,
    x_sem, mask_send, mask_recv, halo_send, halo_recv, tile_send, tile_recv,
    out_ref, out_sem,
):
    band_rows, cols = mask_s.shape
    height = band_rows * side
    width = side * channels
    tiles = band_rows * cols
    quad = 2 * LANES
    groups = width // quad
    per = quad // channels
    half = LANES // channels
    me = lax.axis_index("row")

    barrier = pltpu.get_barrier_semaphore()

    def greet(j, carry):
        pl.semaphore_signal(
            barrier, inc=1, device_id={"row": lax.rem(me + j, n)}, device_id_type=MESH
        )
        return carry

    lax.fori_loop(1, n, greet, 0)

    def fetch(c):
        return pltpu.make_async_copy(
            x_ref.at[:, pl.ds(c * width, width)],
            image.at[pl.ds(PACK, height), pl.ds(LANES + c * width, width)],
            x_sem.at[c],
        )

    for c in range(cols):
        fetch(c).start()

    none = jnp.zeros((channels, channels), jnp.bfloat16)
    for dy in range(3):
        taps = [w_ref[dy, 0], w_ref[dy, 1], w_ref[dy, 2]]
        for p in range(2 * per):
            for q in range(per // half):
                u = p - half - half * q
                parts = [taps[u + 1 - o] if 0 <= u + 1 - o <= 2 else none for o in range(half)]
                wide[dy, p * channels:(p + 1) * channels, q * LANES:(q + 1) * LANES] = (
                    jnp.concatenate(parts, axis=1)
                )
    edge = jnp.zeros((height + 2 * PACK, LANES), jnp.bfloat16)
    image[:, 0:LANES] = edge
    image[:, LANES + cols * width:2 * LANES + cols * width] = edge
    masks[me] = mask_v[...]
    blank_rows = jnp.zeros((PACK, cols * width), jnp.bfloat16)
    image[0:PACK, LANES:LANES + cols * width] = blank_rows
    image[PACK + height:2 * PACK + height, LANES:LANES + cols * width] = blank_rows

    firsts, lasts = [], []
    for c in range(cols):
        fetch(c).wait()
        for r in range(band_rows):
            keep = jnp.full((side, LANES), mask_s[r, c], jnp.int32).astype(jnp.float32)
            keep = keep.astype(jnp.bfloat16)
            for k in range(width // LANES):
                at = (pl.ds(PACK + r * side, side), pl.ds(LANES + c * width + k * LANES, LANES))
                image[at] = image[at] * keep
        span = pl.ds(LANES + c * width, width)
        first = image[PACK:2 * PACK, span].astype(jnp.float32)
        last = image[height:height + PACK, span].astype(jnp.float32)
        firsts.append(first[0:1])
        lasts.append(last[PACK - 1:PACK])
    stage_up[...] = jnp.concatenate(firsts, axis=0).astype(jnp.bfloat16)
    stage_dn[...] = jnp.concatenate(lasts, axis=0).astype(jnp.bfloat16)

    pl.semaphore_wait(barrier, n - 1)

    down = pltpu.make_async_remote_copy(
        stage_dn, halo_top, halo_send.at[0], halo_recv.at[0],
        device_id={"row": lax.rem(me + 1, n)}, device_id_type=MESH)
    up = pltpu.make_async_remote_copy(
        stage_up, halo_bot, halo_send.at[1], halo_recv.at[1],
        device_id={"row": lax.rem(me + n - 1, n)}, device_id_type=MESH)
    is_first = me == 0
    is_last = me == n - 1

    @pl.when(jnp.logical_not(is_last))
    def _():
        down.start()

    @pl.when(jnp.logical_not(is_first))
    def _():
        up.start()

    def mask_copy(target, slot):
        return pltpu.make_async_remote_copy(
            mask_v, masks.at[slot], mask_send.at[target], mask_recv.at[slot],
            device_id={"row": target}, device_id_type=MESH)

    def tell(j, carry):
        mask_copy(lax.rem(me + j, n), me).start()
        return carry

    lax.fori_loop(1, n, tell, 0)

    bias = b_ref[...].astype(jnp.float32)
    bias = jnp.concatenate([bias] * per, axis=1)
    duo = 2
    duos = cols // duo
    bands = duo * groups

    def convolve(r, pair, carry):
        left = pl.multiple_of(pair * (duo * width), duo * width)
        for k in range(bands + 1):
            block = image[r * side:(r + 1) * side + 2 * PACK, pl.ds(left + k * quad, quad)]
            span = pl.ds(k * quad, quad)
            block32 = block.astype(jnp.float32)
            rows3[0, :, span] = block32[PACK - 1:PACK - 1 + side].astype(jnp.bfloat16)
            rows3[1, :, span] = block[PACK:PACK + side]
            rows3[2, :, span] = block32[PACK + 1:PACK + 1 + side].astype(jnp.bfloat16)
        left_side = jnp.concatenate([jnp.concatenate(
            [rows3[dy, :, g * quad:(g + 2) * quad] for g in range(bands)], axis=0)
            for dy in range(3)], axis=1)
        total = jnp.dot(left_side, wide[...].reshape(6 * quad, quad),
            preferred_element_type=jnp.float32) + bias
        done = total.astype(jnp.bfloat16)
        for g in range(bands):
            at = g % groups * quad
            tile_at = r * cols + pair * duo + g // groups
            conv[tile_at, :, at:at + quad] = done[g * side:(g + 1) * side]
            if r == band_rows - 1:
                low[pair * duo + g // groups, :, at:at + quad] = (
                    total[(g + 1) * side - 8:(g + 1) * side])
        return carry

    lax.fori_loop(0, duos, functools.partial(convolve, band_rows - 1), 0)

    @pl.when(jnp.logical_not(is_first))
    def _():
        down.wait_recv()
        lines = halo_top[...].astype(jnp.float32)
        for c in range(cols):
            image[0:PACK, LANES + c * width:LANES + (c + 1) * width] = (
                jnp.broadcast_to(lines[c:c + 1], (PACK, width)).astype(jnp.bfloat16))

    for r in range(band_rows - 2, 0, -1):
        lax.fori_loop(0, duos, functools.partial(convolve, r), 0)
    lax.fori_loop(duos - 1, duos, functools.partial(convolve, 0), 0)

    @pl.when(jnp.logical_not(is_last))
    def _():
        up.wait_recv()
        lines = halo_bot[...].astype(jnp.float32)
        blank = jnp.zeros((1, LANES), jnp.float32)
        before = jnp.concatenate([blank, lines[0:cols - 1, width - LANES:width]], axis=0)
        after = jnp.concatenate([lines[1:cols, 0:LANES], blank], axis=0)
        lines = jnp.concatenate([before, lines, after], axis=1)
        stack = jnp.concatenate(
            [lines[:, g * quad:(g + 2) * quad] for g in range(groups)], axis=0)
        more = jnp.dot(
            stack.astype(jnp.bfloat16), wide[2], preferred_element_type=jnp.float32)
        lowest = lax.broadcasted_iota(jnp.int32, (PACK, quad), 0) == PACK - 1
        for c in range(cols):
            for g in range(groups):
                at = g * quad
                row = low[c, 7:8, at:at + quad] + more[g * cols + c:g * cols + c + 1]
                where = ((band_rows - 1) * cols + c, pl.ds(side - PACK, PACK), pl.ds(at, quad))
                old = conv[where].astype(jnp.float32)
                new = jnp.where(lowest, jnp.broadcast_to(row, (PACK, quad)), old)
                conv[where] = new.astype(jnp.bfloat16)

    seen = []
    for r in range(band_rows):
        for c in range(cols):
            seen.append(mask_s[r, c] + (seen[-1] if seen else 0))

    def place(rank):
        total = jnp.int32(0)
        for count in seen:
            total = total + jnp.where(count <= rank, 1, 0)
        return jnp.minimum(total, tiles - 1)

    def tile(k):
        return pltpu.make_async_remote_copy(
            onward.at[k], arrived.at[k], tile_send.at[k], tile_recv.at[k],
            device_id={"row": lax.rem(me + 1, n)}, device_id_type=MESH)

    for k in range(SHIFT_MOST):
        onward[k] = conv[place(seen[-1] - SHIFT_MOST + k)]

        @pl.when(jnp.logical_not(is_last))
        def _():
            tile(k).start()

    lax.fori_loop(0, duos - 1, functools.partial(convolve, 0), 0)

    def told(j, carry):
        mask_copy(lax.rem(me + j, n), lax.rem(me + j, n)).wait_recv()
        return carry

    lax.fori_loop(1, n, told, 0)
    device = lax.broadcasted_iota(jnp.int32, masks.shape, 0)
    excess = jnp.sum(jnp.where(device < me, masks[...], 0)) - SLOTS * me

    def give(k):
        return pltpu.make_async_copy(out_ref.at[k], out_any.at[k], out_sem.at[k])

    for k in range(SHIFT_MOST, SLOTS):
        out_ref[k] = conv[place(k - excess)]
        give(k).start()
    for k in range(SHIFT_MOST):
        out_ref[k] = conv[place(k - excess)]

    @pl.when(jnp.logical_not(is_first))
    def _():
        for k in range(SHIFT_MOST):
            tile(k).wait_recv()
        late_at = [
            jnp.minimum(k + SHIFT_MOST - jnp.clip(excess, 0, SHIFT_MOST), SHIFT_MOST - 1)
            for k in range(SHIFT_MOST)
        ]
        for k in range(SHIFT_MOST):
            own = out_ref[k].astype(jnp.float32)
            theirs = arrived[late_at[k]].astype(jnp.float32)
            late = jnp.full(own.shape, excess, jnp.int32) > k
            out_ref[k] = jnp.where(late, theirs, own).astype(jnp.bfloat16)
        up.wait_send()

    for k in range(SHIFT_MOST):
        give(k).start()

    @pl.when(jnp.logical_not(is_last))
    def _():
        down.wait_send()
        for k in range(SHIFT_MOST):
            tile(k).wait_send()

    def sent(j, carry):
        mask_copy(lax.rem(me + j, n), me).wait_send()
        return carry

    lax.fori_loop(1, n, sent, 0)
    for k in range(SLOTS):
        give(k).wait()


def hand_on(in_ref, out_ref, held, in_sem, out_sem):
    def take(k):
        return pltpu.make_async_copy(in_ref.at[k], held.at[k], in_sem.at[k])

    def give(k):
        return pltpu.make_async_copy(held.at[k], out_ref.at[k], out_sem.at[k])

    for k in range(SLOTS):
        take(k).start()
    for k in range(SLOTS):
        take(k).wait()
        give(k).start()
    for k in range(SLOTS):
        give(k).wait()


def on_device(slide_pixels, tissue_mask, conv_weight, conv_bias):
    n = lax.axis_size("row")
    band_rows, cols = tissue_mask.shape
    channels = conv_weight.shape[2]
    height = slide_pixels.shape[0]
    side = height // band_rows
    width = side * channels
    quad = 2 * LANES
    vmem = pl.BlockSpec(memory_space=pltpu.VMEM)
    bf16 = jnp.bfloat16
    tiles = pl.pallas_call(
        functools.partial(kernel, n, side, channels),
        out_shape=jax.ShapeDtypeStruct((SLOTS, side, width), bf16),
        in_specs=[
            pl.BlockSpec(memory_space=pl.ANY),
            pl.BlockSpec(memory_space=pltpu.SMEM),
            vmem, vmem, vmem,
        ],
        out_specs=pl.BlockSpec(memory_space=pl.ANY),
        scratch_shapes=[
            pltpu.VMEM((height + 2 * PACK, cols * width + 2 * LANES), bf16),
            pltpu.VMEM((band_rows * cols, side, width), bf16),
            pltpu.VMEM((cols, 8, width), jnp.float32),
            pltpu.VMEM((3, side, 2 * width + quad), bf16),
            pltpu.VMEM((3, 2 * quad, quad), bf16),
            pltpu.VMEM((n, band_rows, cols), jnp.int32),
            pltpu.VMEM((cols, width), bf16),
            pltpu.VMEM((cols, width), bf16),
            pltpu.VMEM((cols, width), bf16),
            pltpu.VMEM((cols, width), bf16),
            pltpu.VMEM((SHIFT_MOST, side, width), bf16),
            pltpu.VMEM((SHIFT_MOST, side, width), bf16),
            pltpu.SemaphoreType.DMA((cols,)),
            pltpu.SemaphoreType.DMA((n,)),
            pltpu.SemaphoreType.DMA((n,)),
            pltpu.SemaphoreType.DMA((2,)),
            pltpu.SemaphoreType.DMA((2,)),
            pltpu.SemaphoreType.DMA((SHIFT_MOST,)),
            pltpu.SemaphoreType.DMA((SHIFT_MOST,)),
            pltpu.VMEM((SLOTS, side, width), bf16),
            pltpu.SemaphoreType.DMA((SLOTS,)),
        ],
        compiler_params=pltpu.CompilerParams(collective_id=0, has_side_effects=True),
    )(slide_pixels, tissue_mask, tissue_mask, conv_weight, conv_bias.reshape(1, channels))
    return pl.pallas_call(
        hand_on,
        out_shape=jax.ShapeDtypeStruct(tiles.shape, bf16),
        in_specs=[pl.BlockSpec(memory_space=pl.ANY)],
        out_specs=pl.BlockSpec(memory_space=pl.ANY),
        scratch_shapes=[
            pltpu.VMEM(tiles.shape, bf16),
            pltpu.SemaphoreType.DMA((SLOTS,)),
            pltpu.SemaphoreType.DMA((SLOTS,)),
        ],
    )(tiles)


def solution(mesh):
    return jax.shard_map(
        on_device,
        mesh=mesh,
        in_specs=(P(("slides", "row"), None), P(("slides", "row"), None), P(), P()),
        out_specs=P(("slides", "row"), None, None),
        check_vma=False,
    )
```
